32 devices in a mesh: dp: 4 (over z), fsdp: 8 (over y, x, core).
Axes of the slice: x: 2, y: 2, z: 4, core: 2. Of those that a mesh axis runs over, the one named last changes fastest.
Arguments:
- x_in: bfloat16 [128, 384, 1536], P(('dp', 'fsdp'))
- positions: int32 [128, 384], P(('dp', 'fsdp'))
- segments: int32 [128, 384], P(('dp', 'fsdp'))
- rel_bias: float32 [32, 16], replicated
- gain_attn: float32 [1536], replicated
- gain_mlp: float32 [1536], replicated
- w_q: bfloat16 [1536, 1024], P('fsdp')
- w_k: bfloat16 [1536, 1024], P('fsdp')
- w_v: bfloat16 [1536, 1024], P('fsdp')
- w_o: bfloat16 [1024, 1536], P('fsdp')
- w_i0: bfloat16 [1536, 3840], P('fsdp')
- w_i1: bfloat16 [1536, 3840], P('fsdp')
- w_f: bfloat16 [3840, 1536], P('fsdp')
- grad_out: bfloat16 [128, 384, 1536], P(('dp', 'fsdp'))
Outputs:
- output 1: bfloat16 [128, 384, 1536], P(('dp', 'fsdp'))
- output 2: float32 [32, 16], replicated
- output 3: float32 [1536], replicated
- output 4: float32 [1536], replicated
- output 5: bfloat16 [1536, 1024], P('fsdp')
- output 6: bfloat16 [1536, 1024], P('fsdp')
- output 7: bfloat16 [1536, 1024], P('fsdp')
- output 8: bfloat16 [1024, 1536], P('fsdp')
- output 9: bfloat16 [1536, 3840], P('fsdp')
- output 10: bfloat16 [1536, 3840], P('fsdp')
- output 11: bfloat16 [3840, 1536], P('fsdp')
All inputs are finite; a program needn't handle non-finite values.
Results may differ from the reference program's by a relative error of at most 0.0194871.
Values are sent between devices in bfloat16 or wider.
A program may use at most 1 GiB of HBM per device.

```python
import jax
import jax.numpy as jnp
from jax import lax

BATCH_ROWS = 128
SEQ_LEN = 384
D_MODEL = 1536
HEADS = 16
HEAD_DIM = 64
FF_DIM = 3840
REL_CLASSES = 32
HALF_CLASSES = REL_CLASSES // 2
EXACT_RANGE = HALF_CLASSES // 2
THRESHOLDS = (12, 16, 23, 32, 46, 64, 91)
EPSILON = 1e-6
NEG_BIG = -1e9


def draw_segments(key):
    margin = SEQ_LEN // 8
    cuts = jax.random.randint(key, (BATCH_ROWS, 2), margin, SEQ_LEN - margin + 1)
    first_cut = jnp.min(cuts, axis=1, keepdims=True)
    second_cut = jnp.max(cuts, axis=1, keepdims=True)
    index = jnp.arange(SEQ_LEN, dtype=jnp.int32)[None, :]
    segments = (index >= first_cut).astype(jnp.int32) + (index >= second_cut).astype(jnp.int32)
    start = jnp.where(segments == 0, 0, jnp.where(segments == 1, first_cut, second_cut))
    positions = (index - start).astype(jnp.int32)
    return positions, segments


def setup_inputs(seed: int = 0) -> dict:
    keys = jax.random.split(jax.random.key(seed), 14)
    width = HEADS * HEAD_DIM
    act_shape = (BATCH_ROWS, SEQ_LEN, D_MODEL)
    score_scale = D_MODEL ** -0.5 * (2.0 / HEAD_DIM) ** 0.25

    def draw_normal(key, shape, scale):
        return jax.random.normal(key, shape, jnp.float32) * scale

    x_in = draw_normal(keys[0], act_shape, 1.0).astype(jnp.bfloat16)
    positions, segments = draw_segments(keys[1])
    rel_bias = draw_normal(keys[2], (REL_CLASSES, HEADS), 1.0)
    gain_attn = 1.0 + draw_normal(keys[3], (D_MODEL,), 0.4)
    gain_mlp = 1.0 + draw_normal(keys[4], (D_MODEL,), 0.4)
    w_q = draw_normal(keys[5], (D_MODEL, width), score_scale).astype(jnp.bfloat16)
    w_k = draw_normal(keys[6], (D_MODEL, width), score_scale).astype(jnp.bfloat16)
    w_v = draw_normal(keys[7], (D_MODEL, width), D_MODEL ** -0.5).astype(jnp.bfloat16)
    w_o = draw_normal(keys[8], (width, D_MODEL), 2.0 * width ** -0.5).astype(jnp.bfloat16)
    w_i0 = draw_normal(keys[9], (D_MODEL, FF_DIM), D_MODEL ** -0.5).astype(jnp.bfloat16)
    w_i1 = draw_normal(keys[10], (D_MODEL, FF_DIM), D_MODEL ** -0.5).astype(jnp.bfloat16)
    w_f = draw_normal(keys[11], (FF_DIM, D_MODEL), 2.0 * FF_DIM ** -0.5).astype(jnp.bfloat16)
    grad_out = draw_normal(keys[12], act_shape, 1.0).astype(jnp.bfloat16)
    return {'x_in': x_in, 'positions': positions, 'segments': segments, 'rel_bias': rel_bias,
            'gain_attn': gain_attn, 'gain_mlp': gain_mlp, 'w_q': w_q, 'w_k': w_k, 'w_v': w_v,
            'w_o': w_o, 'w_i0': w_i0, 'w_i1': w_i1, 'w_f': w_f, 'grad_out': grad_out}


def mat(left, right):
    return jnp.dot(left.astype(jnp.float32), right.astype(jnp.float32))


def rms_norm(values, gain):
    inv_rms = lax.rsqrt(jnp.mean(values * values, axis=-1, keepdims=True) + EPSILON)
    return (values * inv_rms * gain).astype(jnp.bfloat16)


def rel_class(pos_row):
    offset = pos_row[None, :] - pos_row[:, None]
    distance = jnp.abs(offset)
    magnitude = jnp.minimum(distance, EXACT_RANGE)
    for bound in THRESHOLDS:
        magnitude = magnitude + (distance >= bound).astype(jnp.int32)
    return magnitude + HALF_CLASSES * (offset > 0).astype(jnp.int32)


def attend_row(q_row, k_row, v_row, pos_row, seg_row, rel_bias):
    scores = jnp.einsum('qhd,khd->hqk', q_row.astype(jnp.float32), k_row.astype(jnp.float32))
    bias = jnp.transpose(rel_bias[rel_class(pos_row)], (2, 0, 1))
    same_seg = seg_row[:, None] == seg_row[None, :]
    scores = scores + bias + jnp.where(same_seg, 0.0, NEG_BIG)
    attn_prob = jax.nn.softmax(scores, axis=-1)
    context = jnp.einsum('hqk,khd->qhd', attn_prob.astype(jnp.bfloat16).astype(jnp.float32), v_row.astype(jnp.float32))
    return context.astype(jnp.bfloat16)


def layer(x_in, positions, segments, param_set):
    rel_bias, gain_attn, gain_mlp, w_q, w_k, w_v, w_o, w_i0, w_i1, w_f = param_set
    rows, seq_len, width = x_in.shape
    heads = rel_bias.shape[1]
    x_float = x_in.astype(jnp.float32).reshape(rows * seq_len, width)
    normed = rms_norm(x_float, gain_attn)
    q_all = mat(normed, w_q).astype(jnp.bfloat16).reshape(rows, seq_len, heads, -1)
    k_all = mat(normed, w_k).astype(jnp.bfloat16).reshape(rows, seq_len, heads, -1)
    v_all = mat(normed, w_v).astype(jnp.bfloat16).reshape(rows, seq_len, heads, -1)
    row_attend = jax.checkpoint(lambda row_args: attend_row(row_args[0], row_args[1], row_args[2], row_args[3], row_args[4], rel_bias))
    context = lax.map(row_attend, (q_all, k_all, v_all, positions, segments))
    context = context.reshape(rows * seq_len, -1)
    hidden = (x_float + mat(context, w_o)).astype(jnp.bfloat16)
    h_float = hidden.astype(jnp.float32)
    mlp_in = rms_norm(h_float, gain_mlp)
    hidden_act = (jax.nn.silu(mat(mlp_in, w_i0)) * mat(mlp_in, w_i1)).astype(jnp.bfloat16)
    y_out = (h_float + mat(hidden_act, w_f)).astype(jnp.bfloat16)
    return y_out.reshape(rows, seq_len, width)


def reference(x_in, positions, segments, rel_bias, gain_attn, gain_mlp, w_q, w_k, w_v, w_o, w_i0, w_i1, w_f, grad_out):
    param_set = (rel_bias, gain_attn, gain_mlp, w_q, w_k, w_v, w_o, w_i0, w_i1, w_f)
    y_out, pull_back = jax.vjp(lambda params_in: layer(x_in, positions, segments, params_in), param_set)
    grads = pull_back(grad_out)[0]
    return (y_out, grads[0], grads[1], grads[2], grads[3], grads[4], grads[5], grads[6], grads[7], grads[8], grads[9])
```

```python
import jax
import jax.numpy as jnp
from jax import lax
from jax.experimental import pallas as pl
from jax.experimental.pallas import tpu as pltpu
from jax.sharding import PartitionSpec as P


EPSILON = 1e-6
NEG_BIG = -1e9
REL_CLASSES = 32
HALF_CLASSES = 16
EXACT_RANGE = 8
THRESHOLDS = (12, 16, 23, 32, 46, 64, 91)
ROW_AXES = ('dp', 'fsdp')
LANES = 128
HEAD_DIM = 64
VMEM_LIMIT = 56 * 1024 * 1024


def rms_norm(values, gain):
    inv_rms = lax.rsqrt(jnp.mean(values * values, axis=-1, keepdims=True) + EPSILON)
    return (values * inv_rms * gain).astype(jnp.bfloat16)


def project(tokens_in, weight):
    return jnp.einsum('td,de->te', tokens_in, weight, preferred_element_type=jnp.float32)


def contract(left, right, left_dim, right_dim):
    return lax.dot_general(left, right, (((left_dim,), (right_dim,)), ((), ())), preferred_element_type=jnp.float32)


def prepare_row(pos_key, pos_query, seg_key, seg_query, cls_ref, mask_ref):
    offset = pos_key[0] - pos_query[0]
    distance = jnp.abs(offset)
    magnitude = jnp.minimum(distance, EXACT_RANGE)
    for bound in THRESHOLDS:
        magnitude = magnitude + jnp.where(distance >= bound, 1, 0)
    cls_ref[...] = magnitude + jnp.where(offset > 0, HALF_CLASSES, 0)
    mask_ref[...] = jnp.where(seg_key[0] == seg_query[0], 0.0, NEG_BIG)


def probabilities(q_head, k_head, head, table, cls_ref, mask_ref):
    seq_len = q_head.shape[0]
    values = jnp.broadcast_to(table[pl.ds(head, 1), :], (seq_len, LANES))
    bias = jnp.concatenate([jnp.take_along_axis(values, cls_ref[:, start:start + LANES], axis=1)
                            for start in range(0, seq_len, LANES)], axis=1)
    scores = contract(k_head, q_head, 1, 1) + bias + mask_ref[...]
    weights = jnp.exp(scores - jnp.max(scores, axis=0, keepdims=True))
    return weights * (1.0 / jnp.sum(weights, axis=0, keepdims=True))


def pair_slice(ref, block):
    return ref[:, pl.ds(pl.multiple_of(block * LANES, LANES), LANES)]


def attn_forward_kernel(pos_key, pos_query, seg_key, seg_query, table, qkv, context, cls_ref, mask_ref):
    prepare_row(pos_key, pos_query, seg_key, seg_query, cls_ref, mask_ref)
    pairs = context.shape[1] // LANES

    @pl.loop(0, pairs)
    def _(pair):
        q_pair, k_pair, v_pair = [pair_slice(qkv, pair + n * pairs) for n in range(3)]
        outs = []
        for sub in range(2):
            lanes = slice(sub * HEAD_DIM, (sub + 1) * HEAD_DIM)
            prob = probabilities(q_pair[:, lanes], k_pair[:, lanes], 2 * pair + sub, table, cls_ref, mask_ref)
            outs.append(contract(v_pair[:, lanes], prob.astype(jnp.bfloat16), 0, 0))
        block = jnp.concatenate(outs, axis=0).T
        context[:, pl.ds(pl.multiple_of(pair * LANES, LANES), LANES)] = block.astype(jnp.bfloat16)


def attn_backward_kernel(pos_key, pos_query, seg_key, seg_query, table, qkv, d_context, *rest):
    d_q, d_k, d_v, d_bias, cls_ref, mask_ref, ds_ref = rest[-7:]
    prepare_row(pos_key, pos_query, seg_key, seg_query, cls_ref, mask_ref)
    pairs = d_context.shape[1] // LANES
    seq_len = d_context.shape[0]

    @pl.when(pl.program_id(0) == 0)
    def _():
        d_bias[...] = jnp.zeros_like(d_bias)

    @pl.loop(0, pairs)
    def _(pair):
        q_pair, k_pair, v_pair = [pair_slice(qkv, pair + n * pairs) for n in range(3)]
        do_pair = pair_slice(d_context, pair)
        dq_parts, dk_parts, dv_parts = [], [], []
        for sub in range(2):
            lanes = slice(sub * HEAD_DIM, (sub + 1) * HEAD_DIM)
            q_head, k_head, v_head, do_head = q_pair[:, lanes], k_pair[:, lanes], v_pair[:, lanes], do_pair[:, lanes]
            head = 2 * pair + sub
            prob = probabilities(q_head, k_head, head, table, cls_ref, mask_ref)
            dv_parts.append(contract(prob.astype(jnp.bfloat16), do_head, 1, 0))
            d_prob = contract(v_head, do_head, 1, 1)
            d_scores = prob * (d_prob - jnp.sum(d_prob * prob, axis=0, keepdims=True))
            ds_ref[head] = d_scores
            d_low = d_scores.astype(jnp.bfloat16)
            dk_parts.append(contract(d_low, q_head, 1, 0))
            dq_parts.append(contract(k_head, d_low, 0, 0))
        out_lanes = pl.ds(pl.multiple_of(pair * LANES, LANES), LANES)
        d_q[:, out_lanes] = jnp.concatenate(dq_parts, axis=0).T.astype(jnp.bfloat16)
        d_k[:, out_lanes] = jnp.concatenate(dk_parts, axis=1).astype(jnp.bfloat16)
        d_v[:, out_lanes] = jnp.concatenate(dv_parts, axis=1).astype(jnp.bfloat16)

    @pl.loop(0, seq_len // 8)
    def _(group):
        keys = pl.ds(pl.multiple_of(group * 8, 8), 8)
        ds_group = ds_ref[:, keys, :].reshape(-1, seq_len)
        high = ds_group.astype(jnp.bfloat16)
        low = (ds_group - high.astype(jnp.float32)).astype(jnp.bfloat16)
        cls_group = jnp.broadcast_to(cls_ref[keys, :][:, None, :], (8, REL_CLASSES, seq_len))
        onehot = jnp.where(cls_group == lax.broadcasted_iota(jnp.int32, cls_group.shape, 1), 1.0, 0.0)
        onehot = onehot.reshape(8 * REL_CLASSES, seq_len).astype(jnp.bfloat16)
        d_bias[...] += contract(high, onehot, 1, 1) + contract(low, onehot, 1, 1)


def attn_specs(seq_len, heads, width, first=0):
    key_spec = pl.BlockSpec((1, seq_len, 1), lambda row: (row + first, 0, 0))
    query_spec = pl.BlockSpec((1, 1, seq_len), lambda row: (row + first, 0, 0))
    table_spec = pl.BlockSpec((heads, LANES), lambda row: (0, 0))
    return [key_spec, query_spec, key_spec, query_spec, table_spec, pl.BlockSpec((seq_len, 3 * width), lambda row: (row + first, 0))]


def attn_cost(rows, seq_len, heads, products):
    scores = rows * heads * seq_len * seq_len
    return pl.CostEstimate(flops=scores * 600 * products, bytes_accessed=rows * seq_len * 8192, transcendentals=scores)


def attn_scratch(seq_len):
    return [pltpu.VMEM((seq_len, seq_len), jnp.int32), pltpu.VMEM((seq_len, seq_len), jnp.float32)]


def attn_forward(index_args, qkv, heads):
    rows, seq_len = index_args[0].shape[:2]
    width = heads * HEAD_DIM
    return pl.pallas_call(
        attn_forward_kernel,
        grid=(rows,),
        in_specs=attn_specs(seq_len, heads, width),
        out_specs=pl.BlockSpec((seq_len, width), lambda row: (row, 0)),
        out_shape=jax.ShapeDtypeStruct((rows * seq_len, width), jnp.bfloat16),
        scratch_shapes=attn_scratch(seq_len),
        cost_estimate=attn_cost(rows, seq_len, heads, 3),
        compiler_params=pltpu.CompilerParams(vmem_limit_bytes=VMEM_LIMIT),
        name='attn_forward',
    )(*index_args, qkv)


def attn_backward(index_args, qkv, d_context, heads, first, count, held):
    rows, seq_len = index_args[0].shape[:2]
    width = heads * HEAD_DIM
    row_spec = pl.BlockSpec((seq_len, width), lambda row: (row + first, 0))
    acc_shape = (8 * heads, 8 * REL_CLASSES)
    d_q, d_k, d_v, sums = pl.pallas_call(
        attn_backward_kernel,
        grid=(count,),
        in_specs=attn_specs(seq_len, heads, width, first) + [row_spec] + [pl.BlockSpec(memory_space=pl.ANY)] * len(held),
        out_specs=[row_spec] * 3 + [pl.BlockSpec(acc_shape, lambda row: (0, 0))],
        out_shape=[jax.ShapeDtypeStruct((rows * seq_len, width), jnp.bfloat16)] * 3 + [jax.ShapeDtypeStruct(acc_shape, jnp.float32)],
        scratch_shapes=attn_scratch(seq_len) + [pltpu.VMEM((heads, seq_len, seq_len), jnp.float32)],
        input_output_aliases={7 + n: n for n in range(len(held))},
        cost_estimate=attn_cost(count, seq_len, heads, 6),
        compiler_params=pltpu.CompilerParams(vmem_limit_bytes=VMEM_LIMIT),
    )(*index_args, qkv, d_context, *held)
    sums = sums.reshape(heads, 8, 8, REL_CLASSES)
    d_bias = sum(sums[:, lane, lane] for lane in range(8))
    return d_q, d_k, d_v, d_bias.T


def gather_full(part):
    return lax.all_gather(part, 'fsdp', axis=0, tiled=True)


def swap_perm(size, bit):
    return [(index, index ^ bit) for index in range(size)]


def swap(value, axis, size, bit):
    return lax.ppermute(value, axis, swap_perm(size, bit))


def widen(value):
    return value.astype(jnp.float32)


def low(value):
    return value.astype(jnp.bfloat16)


def pick(blocks, index):
    return lax.dynamic_index_in_dim(blocks, index, 0, keepdims=False)


class WeightSum:
    def __init__(self, *grads):
        rank = lax.axis_index('fsdp')
        self.core, self.chip, self.plane = rank & 1, rank >> 1, lax.axis_index('dp')
        self.grads = [grad.reshape(4, 2, grad.shape[0] // 8, grad.shape[1]) for grad in grads]
        other = [lax.dynamic_index_in_dim(grad, 1 - self.core, 1, keepdims=False) for grad in self.grads]
        self.sent = jnp.concatenate([low(part) for part in other], axis=-1)

    def cores(self):
        self.got = swap(self.sent, 'fsdp', 8, 1)

    def chip_block(self, chip):
        own = [lax.dynamic_slice(grad, [chip, self.core, 0, 0], (1, 1) + grad.shape[2:])[0, 0] for grad in self.grads]
        return jnp.concatenate(own, axis=-1) + widen(pick(self.got, chip))

    def chips(self):
        self.sends = [low(self.chip_block(self.chip ^ bits)) for bits in (3, 1, 2)]
        self.received = [swap(block, 'fsdp', 8, 2 * bits) for block, bits in zip(self.sends, (3, 1, 2))]

    def planes(self):
        shard = self.chip_block(self.chip)
        for block in self.received:
            shard = shard + widen(block)
        self.shape = shard.shape
        quarters = shard.reshape(4, shard.shape[0] // 4, shard.shape[1])
        self.rings = [[(i, (i + step) % 4) for i in range(4)] for step in (1, 2, 3)]
        self.pieces = [low(pick(quarters, (self.plane + step) % 4)) for step in (1, 2, 3)]
        self.kept = pick(quarters, self.plane)
        self.parts = [lax.ppermute(piece, 'dp', ring) for piece, ring in zip(self.pieces, self.rings)]

    def spread(self):
        self.total = low(self.kept + widen(self.parts[0]) + widen(self.parts[1]) + widen(self.parts[2]))
        self.others = [lax.ppermute(self.total, 'dp', ring) for ring in self.rings]

    def result(self):
        out = jnp.zeros((4,) + self.total.shape, jnp.bfloat16)
        out = lax.dynamic_update_index_in_dim(out, self.total, self.plane, 0)
        for step in (1, 2, 3):
            out = lax.dynamic_update_index_in_dim(out, self.others[step - 1], (self.plane + 4 - step) % 4, 0)
        return out.reshape(self.shape)


def sum_small(value):
    for axis, size, bit in (('dp', 4, 1), ('dp', 4, 2), ('fsdp', 8, 2), ('fsdp', 8, 4)):
        value = value + swap(value, axis, size, bit)
    return value


def after(value, *others):
    return lax.optimization_barrier((value, others))[0]


def token_grad(left, right):
    return jnp.einsum('tk,tn->kn', left, right, preferred_element_type=jnp.float32)


def back_project(grad, weight):
    return jnp.einsum('tn,kn->tk', grad, weight, preferred_element_type=jnp.float32)


def local_layer(x_in, positions, segments, rel_bias, gain_attn, gain_mlp, wq_part, wk_part, wv_part, wo_part, wi0_part, wi1_part, wf_part, grad_out):
    rows, seq_len, dim = x_in.shape
    classes, heads = rel_bias.shape
    width = wq_part.shape[1]
    ff = wi0_part.shape[1]
    w_qkv = gather_full(jnp.concatenate([wq_part, wk_part, wv_part], axis=1))
    w_o = gather_full(wo_part)
    w_i = gather_full(jnp.concatenate([wi0_part, wi1_part], axis=1))
    w_f = gather_full(wf_part)

    tokens = x_in.reshape(rows * seq_len, dim)
    grad_y = grad_out.reshape(rows * seq_len, dim)
    table = jnp.pad(rel_bias.T, ((0, 0), (0, LANES - classes)))
    index_args = (positions[:, :, None], positions[:, None, :], segments[:, :, None], segments[:, None, :], table)
    x_float = widen(tokens)
    normed, norm1_pull = jax.vjp(lambda gain: rms_norm(x_float, gain), gain_attn)
    qkv = low(project(normed, w_qkv))
    context = attn_forward(index_args, qkv, heads)
    hidden = low(x_float + project(context, w_o))
    h_float = widen(hidden)
    mlp_in, norm2_pull = jax.vjp(rms_norm, h_float, gain_mlp)
    w_i = after(w_i, mlp_in)
    gate = project(mlp_in, w_i[:, :ff])
    up_proj = project(mlp_in, w_i[:, ff:])
    act_float, act_pull = jax.vjp(lambda gate_in, up_in: jax.nn.silu(gate_in) * up_in, gate, up_proj)
    hidden_act = low(act_float)

    sum_f = WeightSum(token_grad(hidden_act, grad_y))
    sum_f.cores()
    d_act = low(back_project(after(grad_y, sum_f.sent), w_f))
    d_gate, d_up = act_pull(widen(d_act))
    d_gate, d_up = low(d_gate), low(d_up)
    sum_f.got = after(sum_f.got, d_gate, d_up)
    sum_f.chips()
    d_gate = after(d_gate, sum_f.sends)
    sum_i0 = WeightSum(token_grad(mlp_in, d_gate))
    sum_i0.cores()
    sum_i1 = WeightSum(token_grad(after(mlp_in, sum_i0.sent), d_up))
    sum_i1.cores()
    sum_i0.got = after(sum_i0.got, sum_i1.sent)
    sum_i0.chips()
    sum_f.received = after(sum_f.received, sum_i0.sends)
    sum_f.planes()
    d_mlp_gate = back_project(after(d_gate, sum_f.pieces), w_i[:, :ff])
    sum_i1.got = after(sum_i1.got, d_mlp_gate)
    sum_i1.chips()
    d_up, d_mlp_gate = after([d_up, d_mlp_gate], sum_i1.sends)
    d_mlp_in = low(d_mlp_gate + back_project(d_up, w_i[:, ff:]))
    d_h_norm, d_gain_mlp = norm2_pull(d_mlp_in)
    d_hidden = low(widen(grad_y) + d_h_norm)
    sum_f.parts = after(sum_f.parts, d_hidden)
    sum_f.spread()
    sum_o = WeightSum(token_grad(context, after(d_hidden, sum_f.total)))
    sum_o.cores()
    d_context = low(back_project(after(d_hidden, sum_o.sent), w_o))
    sum_o.got = after(sum_o.got, d_context)
    sum_o.chips()
    d_context = after(d_context, sum_o.sends)
    half = rows // 2
    d_q, d_k, d_v, d_bias = attn_backward(index_args, qkv, d_context, heads, 0, half, ())
    sum_i0.received = after(sum_i0.received, d_q)
    sum_i0.planes()
    d_context = after(d_context, sum_i0.pieces)
    d_q, d_k, d_v, d_bias_rest = attn_backward(index_args, qkv, d_context, heads, half, rows - half, (d_q, d_k, d_v))
    sum_i0.parts, sum_i1.received, sum_o.received, sum_f.others = after(
        [sum_i0.parts, sum_i1.received, sum_o.received, sum_f.others], d_q)
    sum_i1.planes()
    sum_i0.spread()
    d_q, d_k, d_v = after([d_q, d_k, d_v], sum_i1.pieces, sum_i0.total)
    sum_q = WeightSum(*[token_grad(normed, d_part) for d_part in (d_q, d_k, d_v)])
    sum_q.cores()
    d_q = after(d_q, sum_q.sent)
    d_normed_q = back_project(d_q, w_qkv[:, :width])
    sum_q.got = after(sum_q.got, d_normed_q)
    sum_q.chips()
    sum_o.received = after(sum_o.received, sum_q.sends)
    sum_o.planes()
    d_k, d_normed_q = after([d_k, d_normed_q], sum_q.sends, sum_o.pieces)
    d_normed = low(d_normed_q + back_project(d_k, w_qkv[:, width:2 * width]) + back_project(d_v, w_qkv[:, 2 * width:]))
    d_gain_attn = norm1_pull(d_normed)[0]
    sum_i1.parts, sum_o.parts = after([sum_i1.parts, sum_o.parts], d_gain_attn)
    sum_i1.spread()
    sum_o.spread()
    small = jnp.concatenate([(d_bias + d_bias_rest).reshape(-1), d_gain_attn, d_gain_mlp])
    small_swap = swap(small, 'fsdp', 8, 1)
    y_out = low(h_float + project(after(hidden_act, small, sum_i1.total, sum_o.total), w_f)).reshape(x_in.shape)
    sum_q.received, small_swap, sum_i0.others, sum_i1.others, sum_o.others, sum_f.others = after(
        [sum_q.received, small_swap, sum_i0.others, sum_i1.others, sum_o.others, sum_f.others], y_out)
    sum_q.planes()
    small, sum_i0.others, sum_i1.others, sum_o.others, sum_f.others = after(
        [small, sum_i0.others, sum_i1.others, sum_o.others, sum_f.others], sum_q.pieces)
    small = sum_small(small + small_swap)
    d_wf, d_wi0, d_wi1, d_wo = [part.result() for part in (sum_f, sum_i0, sum_i1, sum_o)]
    sum_q.spread()
    d_wqkv = sum_q.result()
    d_wq, d_wk, d_wv = [d_wqkv[:, n * width:(n + 1) * width] for n in range(3)]
    count = classes * heads
    return (y_out, small[:count].reshape(classes, heads), small[count:count + dim], small[count + dim:],
            d_wq, d_wk, d_wv, d_wo, d_wi0, d_wi1, d_wf)


def solution(mesh):
    row_spec = P(ROW_AXES)
    whole = P()
    part_spec = P('fsdp')
    in_specs = (row_spec, row_spec, row_spec, whole, whole, whole) + (part_spec,) * 7 + (row_spec,)
    out_specs = (row_spec, whole, whole, whole) + (part_spec,) * 7
    return jax.shard_map(local_layer, mesh=mesh, in_specs=in_specs, out_specs=out_specs, check_vma=False)
```
